32 devices in a mesh: fsdp: 8 (over z, core), tp: 4 (over y, x).
Axes of the slice: x: 2, y: 2, z: 4, core: 2. Of those that a mesh axis runs over, the one named last changes fastest.
Arguments:
- hidden: bfloat16 [3072, 7168], P('fsdp'), may hold values from -72 to 72
- w_query: bfloat16 [7168, 4096], P('fsdp', 'tp'), may hold values from -0.0625 to 0.0625
- w_key: bfloat16 [7168, 1024], P('fsdp', 'tp'), may hold values from -0.0625 to 0.0625
- w_value: bfloat16 [7168, 1024], P('fsdp', 'tp'), may hold values from -0.0625 to 0.0625
- w_out: bfloat16 [4096, 7168], P('tp', 'fsdp'), may hold values from -0.09375 to 0.09375
- exp_query: int32 [56, 32], replicated, may hold values from -1 to 1
- exp_key: int32 [56, 8], replicated, may hold values from -1 to 1
- exp_value: int32 [56, 8], replicated, may hold values from -1 to 1
- exp_out: int32 [32, 56], replicated, may hold values from -1 to 1
- owner: int32 [8], replicated, may hold values from 0 to 7, each once
Outputs:
- attended: bfloat16 [3072, 7168], P('fsdp', 'tp')
The draws below stay inside these ranges and needn't reach their ends.
Inputs may be any that keep to these rules, and one draw needn't show every extreme that they name: Trainer shard i holds logical slab owner[i]; every slab is held once.
All inputs are finite; a program needn't handle non-finite values.
Results may differ from the reference program's by a relative error of at most 0.038.
Values may be sent and summed in bfloat16 or wider, within the bound.
A program may use at most 128 MiB of HBM per device.

```python
import math
import jax
import jax.numpy as jnp
from jax import lax

D = 7168
HQ = 32
HK = 8
HD = 128
BLOCK = 128
TOKENS = 3072
QW = 4096
KW = 1024
N_FSDP = 8
N_TP = 4


def draw_hidden(key, part):
    first = jax.random.fold_in(jax.random.fold_in(key, 17), 0)
    values = jnp.clip(jax.random.normal(first, (TOKENS, D), jnp.float32), -6.0, 6.0)
    return values.astype(jnp.bfloat16)


def with_ends(entries, stream_key, least, largest):
    longest = entries.shape.index(max(entries.shape))
    spots = []
    for shift in (0, 1):
        where = [jax.random.randint(jax.random.fold_in(stream_key, axis), (), 0, length) for axis, length in enumerate(entries.shape)]
        where[longest] = (where[longest] + shift) % entries.shape[longest]
        spots.append(tuple(where))
    return entries.at[spots[0]].set(least).at[spots[1]].set(largest)


def level_of(key, extent, cuts, smallest, top_value):
    factor_of, own = 1.0, jax.random.fold_in(key, 6)
    for axis_at, blocks in cuts:
        heights = jnp.exp(jax.random.uniform(jax.random.fold_in(own, axis_at), (blocks,), jnp.float32, smallest / len(cuts), top_value / len(cuts)))
        factor_of = factor_of * jnp.repeat(heights, extent[axis_at] // blocks).reshape([-1 if axis == axis_at else 1 for axis in range(len(extent))])
    return factor_of


def scatter_about(key, dims, spread, reach, pieces=(), held_as=jnp.bfloat16):
    entries = spread * jax.random.normal(key, dims, jnp.float32)
    if pieces:
        entries = entries * level_of(key, dims, pieces, -0.22, 0.18)
    return jnp.clip(entries, -reach, reach).astype(held_as)


def setup_inputs(seed: int = 0) -> dict:
    streams_of = jax.random.split(jax.random.key(seed), 11)
    hidden = draw_hidden(jax.random.fold_in(streams_of[10], 71), 0)
    w_query = scatter_about(streams_of[1], (D, QW), D ** -0.5, 0.0625, ((0, 8), (1, 4)))
    w_key = scatter_about(streams_of[2], (D, KW), D ** -0.5, 0.0625, ((0, 8), (1, 4)))
    w_value = scatter_about(streams_of[3], (D, KW), D ** -0.5, 0.0625, ((0, 8), (1, 4)))
    w_out = scatter_about(streams_of[4], (QW, D), QW ** -0.5, 0.09375, ((0, 4), (1, 8)))
    exp_query = with_ends(jax.random.randint(streams_of[5], (D // BLOCK, QW // BLOCK), -1, 2), jax.random.fold_in(streams_of[5], 1), -1, 1).astype(jnp.int32)
    exp_key = with_ends(jax.random.randint(streams_of[6], (D // BLOCK, KW // BLOCK), -1, 2), jax.random.fold_in(streams_of[6], 1), -1, 1).astype(jnp.int32)
    exp_value = with_ends(jax.random.randint(streams_of[7], (D // BLOCK, KW // BLOCK), -1, 2), jax.random.fold_in(streams_of[7], 1), -1, 1).astype(jnp.int32)
    exp_out = with_ends(jax.random.randint(streams_of[8], (QW // BLOCK, D // BLOCK), -1, 2), jax.random.fold_in(streams_of[8], 1), -1, 1).astype(jnp.int32)
    owner = jax.random.permutation(streams_of[9], N_FSDP).astype(jnp.int32)
    return dict(hidden=hidden, w_query=w_query, w_key=w_key, w_value=w_value, w_out=w_out, exp_query=exp_query, exp_key=exp_key, exp_value=exp_value, exp_out=exp_out, owner=owner)


neg_large = -1e+30

def dequantize(weight, exponents):
    block_size = weight.shape[0] // exponents.shape[0]
    factor = jnp.exp2(exponents.astype(jnp.float32))
    factor = jnp.repeat(jnp.repeat(factor, block_size, axis=0), block_size, axis=1)
    return (weight.astype(jnp.float32) * factor).astype(jnp.bfloat16)

def reference(hidden, w_query, w_key, w_value, w_out, exp_query, exp_key, exp_value, exp_out, owner):
    slab_rows = D // N_FSDP
    inverse = jnp.argsort(owner).astype(jnp.int32)

    def rows_logical(weight):
        shaped = weight.reshape(N_FSDP, slab_rows, weight.shape[1])
        return jnp.take(shaped, inverse, axis=0).reshape(weight.shape)

    def cols_logical(weight):
        shaped = weight.reshape(weight.shape[0], N_FSDP, slab_rows)
        return jnp.take(shaped, inverse, axis=1).reshape(weight.shape)
    query_w = dequantize(rows_logical(w_query), exp_query)
    key_w = dequantize(rows_logical(w_key), exp_key)
    value_w = dequantize(rows_logical(w_value), exp_value)
    out_w = dequantize(cols_logical(w_out), exp_out)
    query = jnp.dot(hidden, query_w, preferred_element_type=jnp.float32).astype(jnp.bfloat16)
    key_all = jnp.dot(hidden, key_w, preferred_element_type=jnp.float32).astype(jnp.bfloat16)
    value_all = jnp.dot(hidden, value_w, preferred_element_type=jnp.float32).astype(jnp.bfloat16)
    tokens = hidden.shape[0]
    group_size = HQ // HK
    query_heads = query.reshape(tokens, HQ, HD).transpose(1, 0, 2)
    key_heads = key_all.reshape(tokens, HK, HD).transpose(1, 0, 2)
    value_heads = value_all.reshape(tokens, HK, HD).transpose(1, 0, 2)
    position = jnp.arange(tokens, dtype=jnp.int32)
    causal = position[:, None] >= position[None, :]
    inv_root = 1.0 / math.sqrt(HD)

    def one_head(head_index):
        query_one = query_heads[head_index]
        key_one = key_heads[head_index // group_size]
        value_one = value_heads[head_index // group_size]
        scores = jnp.dot(query_one, key_one.T, preferred_element_type=jnp.float32) * inv_root
        scores = jnp.where(causal, scores, neg_large)
        row_top = lax.optimization_barrier(jnp.max(scores, axis=1, keepdims=True))
        weights = jnp.where(causal, jnp.exp(scores - row_top), 0.0)
        row_total = lax.optimization_barrier(jnp.sum(weights, axis=1, keepdims=True))
        mixed_sum = jnp.dot(weights.astype(jnp.bfloat16), value_one, preferred_element_type=jnp.float32)
        return (mixed_sum / row_total).astype(jnp.bfloat16)
    context = lax.map(one_head, jnp.arange(HQ, dtype=jnp.int32))
    context = context.transpose(1, 0, 2).reshape(tokens, HQ * HD)
    rows_tp = HQ * HD // N_TP
    attended = jnp.zeros((tokens, D), jnp.float32)
    for tp_rank in range(N_TP):
        part_sum = jnp.dot(context[:, tp_rank * rows_tp:(tp_rank + 1) * rows_tp], out_w[tp_rank * rows_tp:(tp_rank + 1) * rows_tp], preferred_element_type=jnp.float32)
        rounded = lax.optimization_barrier(part_sum.astype(jnp.bfloat16))
        attended = attended + rounded.astype(jnp.float32)
    return attended.astype(jnp.bfloat16)
```

```python
from functools import partial
import math

import jax
import jax.numpy as jnp
from jax import lax
from jax.experimental import pallas as pl
from jax.experimental.pallas import tpu as pltpu
from jax.sharding import PartitionSpec as P

HQ = 32
HK = 8
HD = 128


neg_large = -1e30


def block_factor(exponents, row_start, row_count, col_start, col_count, block_size):
    repeated = jnp.repeat(exponents, block_size, axis=0)
    picked = lax.dynamic_slice_in_dim(repeated, row_start, row_count, 0)
    repeated = jnp.repeat(picked, block_size, axis=1)
    picked = lax.dynamic_slice_in_dim(repeated, col_start, col_count, 1)
    return jnp.exp2(picked.astype(jnp.float32))


def block_update(state, query_half, pos_half, keys_part, values_part, key_pos, inv_root):
    row_max, row_sum, accum = state
    causal = pos_half[:, None] >= key_pos[None, :]
    scores = (
        jnp.einsum("tgjd,ngd->gjtn", query_half, keys_part, preferred_element_type=jnp.float32)
        * inv_root
    )
    scores = jnp.where(causal, scores, neg_large)
    new_max = jnp.maximum(row_max, jnp.max(scores, axis=3))
    rescale = jnp.exp(row_max - new_max)
    weights = jnp.where(causal, jnp.exp(scores - new_max[..., None]), 0.0)
    row_sum = row_sum * rescale + jnp.sum(weights, axis=3)
    accum = accum * rescale[..., None] + jnp.einsum(
        "gjtn,ngd->gjtd",
        weights.astype(jnp.bfloat16),
        values_part,
        preferred_element_type=jnp.float32,
    )
    return (new_max, row_sum, accum)


def keep_state(state):
    return state


def gather_body(hidden, w_query, w_key, w_value, w_out, exp_query, exp_key, exp_value, exp_out, owner):
    fsdp_index = lax.axis_index("fsdp")
    tp_index = lax.axis_index("tp")
    slab_rows = w_query.shape[0]
    groups = owner.shape[0]
    tokens = hidden.shape[0]
    model_width = hidden.shape[1]
    block_size = model_width // exp_query.shape[0]
    slab_start = owner[fsdp_index] * slab_rows
    query_cols = w_query.shape[1]
    key_cols = w_key.shape[1]

    def scaled_rows(weight, exponents):
        col_count = weight.shape[1]
        factor = block_factor(
            exponents, slab_start, slab_rows, tp_index * col_count, col_count, block_size
        )
        return (weight.astype(jnp.float32) * factor).astype(jnp.bfloat16)

    query_local = scaled_rows(w_query, exp_query)
    key_local = scaled_rows(w_key, exp_key)
    value_local = scaled_rows(w_value, exp_value)
    out_rows = w_out.shape[0]
    out_factor = block_factor(
        exp_out, tp_index * out_rows, out_rows, slab_start, slab_rows, block_size
    )
    out_local = (w_out.astype(jnp.float32) * out_factor).astype(jnp.bfloat16)
    arranged = jnp.take(hidden.reshape(tokens, groups, slab_rows), owner, axis=1).reshape(
        tokens, model_width
    )
    pieces = (
        lax.all_gather(query_local, "fsdp", axis=0, tiled=True),
        lax.all_gather(key_local, "fsdp", axis=0, tiled=True),
        lax.all_gather(value_local, "fsdp", axis=0, tiled=True),
    )
    query_sum, key_sum, value_sum = tuple(
        (jnp.dot(arranged, weight, preferred_element_type=jnp.float32) for weight in pieces)
    )
    query = query_sum.astype(jnp.bfloat16)
    key_here = key_sum.astype(jnp.bfloat16)
    value_here = value_sum.astype(jnp.bfloat16)
    half_rows = tokens // 2
    local_pos = fsdp_index * tokens + jnp.arange(tokens, dtype=jnp.int32)
    group_size = HQ // HK
    kv_heads = key_cols // HD
    query_halves = query.reshape(2, half_rows, kv_heads, group_size, HD)
    pos_halves = local_pos.reshape(2, half_rows)
    pos_top = jnp.max(pos_halves, axis=1)
    inv_root = 1.0 / math.sqrt(HD)
    one_state = (
        jnp.full((kv_heads, group_size, half_rows), neg_large, jnp.float32),
        jnp.zeros((kv_heads, group_size, half_rows), jnp.float32),
        jnp.zeros((kv_heads, group_size, half_rows, HD), jnp.float32),
    )
    offset = jnp.int32(0)
    key_piece = lax.all_gather(key_here, "fsdp", axis=0, tiled=True)
    value_piece = lax.all_gather(value_here, "fsdp", axis=0, tiled=True)
    states = list((one_state, one_state))
    piece_rows = key_piece.shape[0]
    for block_low in range(0, piece_rows, 1024):
        block_high = min(block_low + 1024, piece_rows)
        width_here = block_high - block_low
        keys_part = key_piece[block_low:block_high].reshape(width_here, kv_heads, HD)
        values_part = value_piece[block_low:block_high].reshape(width_here, kv_heads, HD)
        key_pos = offset + block_low + jnp.arange(width_here, dtype=jnp.int32)
        for attend_which in range(2):
            update = partial(
                block_update,
                query_half=query_halves[attend_which],
                pos_half=pos_halves[attend_which],
                keys_part=keys_part,
                values_part=values_part,
                key_pos=key_pos,
                inv_root=inv_root,
            )
            states[attend_which] = lax.cond(
                offset + block_low <= pos_top[attend_which],
                update,
                keep_state,
                states[attend_which],
            )
    final_states = tuple(states)
    context_parts = []
    for which in range(2):
        row_max, row_sum, accum = final_states[which]
        part_context = (accum / row_sum[..., None]).astype(jnp.bfloat16)
        context_parts.append(part_context.transpose(2, 0, 1, 3).reshape(half_rows, query_cols))
    context = jnp.concatenate(context_parts, axis=0)
    column_terms = jnp.dot(
        context,
        lax.all_gather(out_local, "fsdp", axis=1, tiled=True),
        preferred_element_type=jnp.float32,
    )
    slab_ids = jnp.arange(groups, dtype=jnp.int32)
    inverse = jnp.sum(
        slab_ids[:, None] * (owner[:, None] == slab_ids[None, :]).astype(jnp.int32), axis=0
    )
    ordered = jnp.take(column_terms.reshape(tokens, groups, slab_rows), inverse, axis=1).reshape(
        tokens, model_width
    )
    result = lax.psum_scatter(ordered.astype(jnp.bfloat16), "tp", scatter_dimension=1, tiled=True)
    return result


MESH = pl.DeviceIdType.MESH
VMEM = pltpu.VMEM


def greet(peers):
    barrier = pltpu.get_barrier_semaphore()
    for device in peers:
        pl.semaphore_signal(barrier, inc=1, device_id=device, device_id_type=MESH)
    pl.semaphore_wait(barrier, len(peers))


def near_first(n):
    steps = []
    for d in range(1, n // 2 + 1):
        steps.append(d)
        if n - d != d:
            steps.append(n - d)
    return steps


def spread_kernel(n_f, n_t, piece_ref, out_ref, send_one, send_two, recv, local_sem):
    f = lax.axis_index("fsdp")
    t = lax.axis_index("tp")
    far = [lax.rem(f + d, n_f) for d in range(n_f)]
    side = [lax.rem(t + k, n_t) for k in range(n_t)]
    greet([{"fsdp": far[d]} for d in range(1, n_f)] + [{"tp": side[k]} for k in range(1, n_t)])
    own = pltpu.make_async_copy(piece_ref.at[f], out_ref.at[f, t], local_sem)
    own.start()
    copies = []
    order = near_first(n_f)
    for d in order:
        copies.append(
            pltpu.make_async_remote_copy(
                src_ref=piece_ref.at[far[d]],
                dst_ref=out_ref.at[f, t],
                send_sem=send_one.at[d],
                recv_sem=recv.at[f, t],
                device_id={"fsdp": far[d]},
                device_id_type=MESH,
            )
        )
        copies[-1].start()

    def forward(slot, source, from_f):
        for k in range(1, n_t):
            copies.append(
                pltpu.make_async_remote_copy(
                    src_ref=source,
                    dst_ref=out_ref.at[from_f, t],
                    send_sem=send_two.at[slot, k],
                    recv_sem=recv.at[from_f, t],
                    device_id={"tp": side[k]},
                    device_id_type=MESH,
                )
            )
            copies[-1].start()

    def arrived(from_f, from_t):
        pltpu.make_async_remote_copy(
            src_ref=piece_ref.at[0],
            dst_ref=out_ref.at[from_f, from_t],
            send_sem=send_one.at[0],
            recv_sem=recv.at[from_f, from_t],
            device_id={"tp": side[1]},
            device_id_type=MESH,
        ).wait_recv()

    forward(0, piece_ref.at[f], f)
    for d in order:
        source = lax.rem(f - d + n_f, n_f)
        arrived(source, t)
        forward(d, out_ref.at[source, t], source)
    for d in [0] + order:
        for k in range(1, n_t):
            arrived(lax.rem(f - d + n_f, n_f), lax.rem(t - k + n_t, n_t))
    for copy in copies:
        copy.wait_send()
    own.wait()


def spread(pieces, n_f, n_t):
    _, rows, cols = pieces.shape
    return pl.pallas_call(
        partial(spread_kernel, n_f, n_t),
        out_shape=jax.ShapeDtypeStruct((n_f, n_t, rows, cols), pieces.dtype),
        in_specs=[pl.BlockSpec(memory_space=VMEM)],
        out_specs=pl.BlockSpec(memory_space=VMEM),
        scratch_shapes=[
            pltpu.SemaphoreType.DMA((n_f,)),
            pltpu.SemaphoreType.DMA((n_f, n_t)),
            pltpu.SemaphoreType.DMA((n_f, n_t)),
            pltpu.SemaphoreType.DMA,
        ],
        compiler_params=pltpu.CompilerParams(collective_id=0, has_side_effects=True),
        name="spread_hidden",
    )(pieces)


def exchange_kernel(n, axis, piece_ref, out_ref, send, recv, local_sem):
    me = lax.axis_index(axis)
    peers = [lax.rem(me + d, n) for d in range(n)]
    greet([{axis: peers[d]} for d in range(1, n)])
    own = pltpu.make_async_copy(piece_ref.at[me], out_ref.at[me], local_sem)
    own.start()
    copies = []
    for d in near_first(n):
        copies.append(
            pltpu.make_async_remote_copy(
                src_ref=piece_ref.at[peers[d]],
                dst_ref=out_ref.at[me],
                send_sem=send.at[d],
                recv_sem=recv.at[me],
                device_id={axis: peers[d]},
                device_id_type=MESH,
            )
        )
        copies[-1].start()
    for d in near_first(n):
        source = lax.rem(me - d + n, n)
        pltpu.make_async_remote_copy(
            src_ref=piece_ref.at[0],
            dst_ref=out_ref.at[source],
            send_sem=send.at[0],
            recv_sem=recv.at[source],
            device_id={axis: peers[1]},
            device_id_type=MESH,
        ).wait_recv()
    for copy in copies:
        copy.wait_send()
    own.wait()


def exchange(pieces, n, axis, collective_id):
    return pl.pallas_call(
        partial(exchange_kernel, n, axis),
        out_shape=jax.ShapeDtypeStruct(pieces.shape, pieces.dtype),
        in_specs=[pl.BlockSpec(memory_space=VMEM)],
        out_specs=pl.BlockSpec(memory_space=VMEM),
        scratch_shapes=[
            pltpu.SemaphoreType.DMA((n,)),
            pltpu.SemaphoreType.DMA((n,)),
            pltpu.SemaphoreType.DMA,
        ],
        compiler_params=pltpu.CompilerParams(collective_id=collective_id, has_side_effects=True),
        name="exchange_" + axis,
    )(pieces)


def scale_into(out_ref, w_ref, fac_ref, at, blocks, block):
    for b in range(blocks):
        rows = slice(b * block, (b + 1) * block)
        for c in range(0, w_ref.shape[1], block):
            cols = slice(at + c, at + c + block)
            weight = w_ref[rows, c : c + block].astype(jnp.float32)
            out_ref[rows, cols] = (weight * fac_ref[b : b + 1, cols]).astype(jnp.bfloat16)


def project_kernel(heads, kv_heads, share, block, h_ref, wq_ref, wk_ref, wv_ref, fac_ref, out_ref, w_scr):
    q_cols = wq_ref.shape[1]
    k_cols = wk_ref.shape[1]
    blocks = wq_ref.shape[0] // block

    @pl.when(pl.program_id(0) == 0)
    def _():
        scale_into(w_scr, wq_ref, fac_ref, 0, blocks, block)
        scale_into(w_scr, wk_ref, fac_ref, q_cols, blocks, block)
        scale_into(w_scr, wv_ref, fac_ref, q_cols + k_cols, blocks, block)

    rows = h_ref.shape[0]
    part = rows // share
    both = jnp.dot(h_ref[...], w_scr[:, :], preferred_element_type=jnp.float32).astype(jnp.bfloat16)
    for j in range(heads):
        g, p = j // share, j % share
        out_ref[j, 0, :rows, :] = both[:, j * HD : (j + 1) * HD]
        span = slice(p * part, (p + 1) * part)
        k_at = q_cols + g * HD
        v_at = q_cols + k_cols + g * HD
        out_ref[j, 0, rows : rows + part, :] = both[span, k_at : k_at + HD]
        out_ref[j, 0, rows + part :, :] = both[span, v_at : v_at + HD]


def attend_kernel(inv_root, key_rows, q_ref, k_ref, v_ref, out_ref):
    i = pl.program_id(0)
    rows = q_ref.shape[0]
    query = q_ref[...]

    def step(j, state, masked):
        row_max, row_sum, accum = state
        at = pl.ds(pl.multiple_of(j * key_rows, key_rows), key_rows)
        scores = (
            lax.dot_general(
                query, k_ref[at, :], (((1,), (1,)), ((), ())), preferred_element_type=jnp.float32
            )
            * inv_root
        )
        if masked:
            q_pos = lax.broadcasted_iota(jnp.int32, scores.shape, 0)
            k_pos = lax.broadcasted_iota(jnp.int32, scores.shape, 1)
            scores = jnp.where(q_pos >= k_pos, scores, neg_large)
        new_max = jnp.maximum(row_max, jnp.max(scores, axis=1, keepdims=True))
        rescale = jnp.exp(row_max - new_max)
        weights = jnp.exp(scores - new_max)
        row_sum = row_sum * rescale + jnp.sum(weights, axis=1, keepdims=True)
        accum = accum * rescale + jnp.dot(
            weights.astype(jnp.bfloat16), v_ref[at, :], preferred_element_type=jnp.float32
        )
        return (new_max, row_sum, accum)

    state = (
        jnp.full((rows, 1), neg_large, jnp.float32),
        jnp.zeros((rows, 1), jnp.float32),
        jnp.zeros((rows, HD), jnp.float32),
    )
    state = step(i, state, True)
    _, row_sum, accum = lax.fori_loop(0, i, lambda j, s: step(j, s, False), state)
    out_ref[...] = (accum / row_sum).astype(jnp.bfloat16)


def out_kernel(heads, block, n_t, c_ref, w_ref, fac_ref, out_ref, w_scr):
    blocks = w_ref.shape[0] // block

    @pl.when(pl.program_id(0) == 0)
    def _():
        w_scr[...] = jnp.zeros_like(w_scr)
        scale_into(w_scr, w_ref, fac_ref, 0, blocks, block)

    context = jnp.concatenate([c_ref[h] for h in range(heads)], axis=1)
    part = jnp.dot(context, w_scr[...], preferred_element_type=jnp.float32).astype(jnp.bfloat16)
    quarter, slab = out_ref.shape[2], out_ref.shape[3]
    for r in range(n_t):
        out_ref[r, 0, :, :] = part[r * quarter : (r + 1) * quarter, :slab]


def stationary_body(
    n_f, n_t, hidden, w_query, w_key, w_value, w_out, exp_query, exp_key, exp_value, exp_out, owner
):
    f = lax.axis_index("fsdp")
    t = lax.axis_index("tp")
    here, width = hidden.shape
    slab = w_query.shape[0]
    tokens = here * n_f
    block = width // exp_query.shape[0]
    slab_blocks = slab // block
    q_cols, k_cols = w_query.shape[1], w_key.shape[1]
    heads, kv_heads = q_cols // HD, k_cols // HD
    share = heads // kv_heads
    quarter = here // n_t
    logical = owner[f]

    def factors(exponents, cols):
        picked = lax.dynamic_slice(
            exponents, (logical * slab_blocks, t * (cols // block)), (slab_blocks, cols // block)
        )
        return jnp.repeat(jnp.exp2(picked.astype(jnp.float32)), block, axis=1)

    in_factor = jnp.concatenate(
        [factors(exp_query, q_cols), factors(exp_key, k_cols), factors(exp_value, k_cols)], axis=1
    )
    out_rows = w_out.shape[0] // block
    out_factor = jnp.repeat(
        jnp.exp2(
            lax.dynamic_slice(
                exp_out, (t * out_rows, logical * slab_blocks), (out_rows, slab_blocks)
            ).astype(jnp.float32)
        ),
        block,
        axis=1,
    )

    in_factor = jnp.pad(in_factor, ((0, -slab_blocks % 8), (0, 0)))
    out_factor = jnp.pad(out_factor, ((0, -out_rows % 8), (0, -slab % 256)))

    mine = lax.dynamic_slice_in_dim(hidden, t * quarter, quarter, 0)
    pieces = jnp.stack(
        [lax.dynamic_slice_in_dim(mine, owner[i] * slab, slab, 1) for i in range(n_f)]
    )
    arranged = spread(pieces, n_f, n_t).reshape(tokens, slab)

    steps = share
    rows = tokens // steps
    part = rows // share
    whole = lambda a: pl.BlockSpec(a.shape, lambda i: (0,) * a.ndim)
    packed = pl.pallas_call(
        partial(project_kernel, heads, kv_heads, share, block),
        grid=(steps,),
        out_shape=jax.ShapeDtypeStruct((heads, steps, rows + 2 * part, HD), jnp.bfloat16),
        in_specs=[
            pl.BlockSpec((rows, slab), lambda i: (i, 0)),
            whole(w_query),
            whole(w_key),
            whole(w_value),
            whole(in_factor),
        ],
        out_specs=pl.BlockSpec((heads, 1, rows + 2 * part, HD), lambda i: (0, i, 0, 0)),
        scratch_shapes=[pltpu.VMEM((slab, q_cols + 2 * k_cols), jnp.bfloat16)],
        compiler_params=pltpu.CompilerParams(vmem_limit_bytes=56 * 1024 * 1024),
        name="project",
    )(arranged, w_query, w_key, w_value, in_factor)
    summed = lax.psum_scatter(packed, "fsdp", scatter_dimension=0, tiled=False)

    groups = [[g * share + p for p in range(share)] for g in range(kv_heads)]
    kv = lax.all_gather(
        summed[:, rows:, :].reshape(steps, 2, part, HD),
        "fsdp",
        axis=1,
        tiled=False,
        axis_index_groups=groups,
    )
    kv = kv.transpose(2, 0, 1, 3, 4).reshape(2, tokens, HD)
    query = summed[:, :rows, :].reshape(tokens, HD)
    tile = here
    context = pl.pallas_call(
        partial(attend_kernel, 1.0 / math.sqrt(HD), tile),
        grid=(tokens // tile,),
        out_shape=jax.ShapeDtypeStruct((tokens, HD), jnp.bfloat16),
        in_specs=[
            pl.BlockSpec((tile, HD), lambda i: (i, 0)),
            pl.BlockSpec((pl.squeezed, tokens, HD), lambda i: (0, 0, 0)),
            pl.BlockSpec((pl.squeezed, tokens, HD), lambda i: (1, 0, 0)),
        ],
        out_specs=pl.BlockSpec((tile, HD), lambda i: (i, 0)),
        compiler_params=pltpu.CompilerParams(vmem_limit_bytes=48 * 1024 * 1024),
        name="attend",
    )(query, kv, kv)

    gathered = lax.all_gather(context, "fsdp", axis=0, tiled=False)
    parts = pl.pallas_call(
        partial(out_kernel, heads, block, n_t),
        grid=(n_f,),
        out_shape=jax.ShapeDtypeStruct((n_t, n_f, quarter, slab), jnp.bfloat16),
        in_specs=[
            pl.BlockSpec((heads, here, HD), lambda i: (0, i, 0)),
            whole(w_out),
            whole(out_factor),
        ],
        out_specs=pl.BlockSpec((n_t, 1, quarter, slab), lambda i: (0, i, 0, 0)),
        scratch_shapes=[pltpu.VMEM((w_out.shape[0], slab + -slab % 256), jnp.bfloat16)],
        compiler_params=pltpu.CompilerParams(vmem_limit_bytes=48 * 1024 * 1024),
        name="project_out",
    )(gathered, w_out, out_factor)
    total = lax.psum_scatter(parts, "tp", scatter_dimension=0, tiled=False)

    by_slab = exchange(total, n_f, "fsdp", 1)
    slab_ids = jnp.arange(n_f, dtype=jnp.int32)
    inverse = jnp.sum(
        slab_ids[:, None] * (owner[:, None] == slab_ids[None, :]).astype(jnp.int32), axis=0
    )
    per = n_f // n_t
    columns = jnp.stack(
        [
            jnp.concatenate([by_slab[inverse[r * per + c]] for c in range(per)], axis=1)
            for r in range(n_t)
        ]
    )
    return exchange(columns, n_t, "tp", 2).reshape(here, width // n_t)


def solution(mesh):
    n_f, n_t = mesh.shape["fsdp"], mesh.shape["tp"]

    def body(*arrays):
        hidden, w_query, w_key = arrays[0], arrays[1], arrays[2]
        heads, kv_heads = w_query.shape[1] // HD, w_key.shape[1] // HD
        fits = heads == n_f and n_f % n_t == 0 and hidden.shape[0] % (16 * n_t) == 0
        if fits:
            return stationary_body(n_f, n_t, *arrays)
        return gather_body(*arrays)

    placed = (
        P("fsdp", None),
        P("fsdp", "tp"),
        P("fsdp", "tp"),
        P("fsdp", "tp"),
        P("tp", "fsdp"),
        P(),
        P(),
        P(),
        P(),
        P(),
    )
    return jax.shard_map(
        body, mesh=mesh, in_specs=placed, out_specs=P("fsdp", "tp"), check_vma=False
    )
```
